32 devices in a mesh: dp: 8 (over z, y), tensor: 4 (over x, core).
Axes of the slice: x: 2, y: 2, z: 4, core: 2. Of those that a mesh axis runs over, the one named last changes fastest.
Arguments:
- tokens: bfloat16 [16384, 768], P('dp'), may hold values from -6 to 6
- cotangent: bfloat16 [16384, 768], P('dp'), may hold values from -6 to 6
- counts: int32 [16, 5], P('dp'), may hold values from 0 to 576, as said below
- sides: int32 [16, 5], P('dp'), may hold values from 0 to 24, as said below
- segments: int32 [16384], P('dp'), may hold values from 0 to 5, as said below
- norm1_gain: float32 [768], replicated, may hold values from 0.5 to 1.5
- norm1_shift: float32 [768], replicated, may hold values from -3 to 3
- w_qkv: bfloat16 [768, 3, 768], P(None, None, 'tensor'), may hold values from -0.21875 to 0.21875
- b_qkv: float32 [3, 768], P(None, 'tensor'), may hold values from -3 to 3
- freqs: float32 [12, 2, 32], P('tensor'), may hold values from -2 to 2
- w_out: bfloat16 [768, 768], P('tensor'), may hold values from -1.5 to 1.5
- b_out: float32 [768], replicated, may hold values from -3 to 3
- norm2_gain: float32 [768], replicated, may hold values from 0.5 to 1.5
- norm2_shift: float32 [768], replicated, may hold values from -3 to 3
- w_fc1: bfloat16 [768, 3072], P(None, 'tensor'), may hold values from -0.21875 to 0.21875
- b_fc1: float32 [3072], P('tensor'), may hold values from -3 to 3
- w_fc2: bfloat16 [3072, 768], P('tensor'), may hold values from -0.109375 to 0.109375
- b_fc2: float32 [768], replicated, may hold values from -3 to 3
Outputs:
- block_output: bfloat16 [16384, 768], P('dp')
- token_grad: float32 [16384, 768], P('dp')
- norm1_gain_grad: float32 [768], replicated
- norm1_shift_grad: float32 [768], replicated
- qkv_grad: float32 [768, 3, 768], P(None, None, 'tensor')
- qkv_bias_grad: float32 [3, 768], P(None, 'tensor')
- freqs_grad: float32 [12, 2, 32], P('tensor')
- out_grad: float32 [768, 768], P('tensor')
- out_bias_grad: float32 [768], replicated
- norm2_gain_grad: float32 [768], replicated
- norm2_shift_grad: float32 [768], replicated
- fc1_grad: float32 [768, 3072], P(None, 'tensor')
- fc1_bias_grad: float32 [3072], P('tensor')
- fc2_grad: float32 [3072, 768], P('tensor')
- fc2_bias_grad: float32 [768], replicated
The draws below stay inside these ranges and needn't reach their ends.
Inputs may be any that keep to these rules, and one draw needn't show every extreme that they name: `counts`: A used image slot holds the square of its side; unused slots hold 0 and come after the used ones; a pack's total is under 1024. `sides`: side of each image's square patch grid; 0 for an unused slot. `segments`: each image lies whole in its pack from the pack's first slot on, in slot order and row-major patch order; slots after the last image hold 5 (padding).
All inputs are finite; a program needn't handle non-finite values.
Results may differ from the reference program's by a relative error of at most 0.014.
Values may be sent and summed in bfloat16 or wider, within the bound.
A program may use at most 128 MiB of HBM per device.

```python
import jax
import jax.numpy as jnp
import numpy as np
from jax import lax

D = 768
H = 12
HD = 64
FF = 3072
PACK = 1024
PACKS = 16
TOKENS = 16384


def pack_layout(key):
    if PACK >= 1024:
        count_rows = np.array([[576, 400, 0, 0, 0], [400, 400, 196, 0, 0], [576, 196, 196, 0, 0], [196, 196, 196, 196, 196], [400, 196, 196, 196, 0]], np.int32)
        side_rows = np.array([[24, 20, 0, 0, 0], [20, 20, 14, 0, 0], [24, 14, 14, 0, 0], [14, 14, 14, 14, 14], [20, 14, 14, 14, 0]], np.int32)
    else:
        count_rows = np.array([[36, 25, 0, 0, 0], [25, 16, 16, 0, 0], [36, 9, 9, 9, 0], [16, 16, 16, 9, 0], [25, 16, 9, 9, 0]], np.int32)
        side_rows = np.array([[6, 5, 0, 0, 0], [5, 4, 4, 0, 0], [6, 3, 3, 3, 0], [4, 4, 4, 3, 0], [5, 4, 3, 3, 0]], np.int32)
    choose = jax.random.randint(jax.random.fold_in(key, 11), (PACKS,), 0, 5)
    choose = choose.at[0].set(0)
    return (jnp.asarray(count_rows)[choose], jnp.asarray(side_rows)[choose])


def draw_counts(key, part):
    return pack_layout(key)[0]


def draw_sides(key, part):
    return pack_layout(key)[1]


def draw_segments(key, part):
    image_counts = pack_layout(key)[0]
    image_ends = jnp.cumsum(image_counts, axis=1, dtype=jnp.int32)
    slot_ids = jnp.arange(PACK, dtype=jnp.int32)
    segment_ids = jnp.sum((slot_ids[None, :, None] >= image_ends[:, None, :]).astype(jnp.int32), axis=-1, dtype=jnp.int32)
    return segment_ids.reshape(TOKENS)


def shard_levels(rng, dims, split, smallest, largest):
    def one(dim, shards_of):
        heights = jax.random.uniform(jax.random.fold_in(jax.random.fold_in(rng, 6), dim), (shards_of,), jnp.float32, smallest / len(split), largest / len(split))
        return jnp.repeat(jnp.exp(heights), dims[dim] // shards_of).reshape((-1,) + (1,) * (len(dims) - dim - 1))

    factor_of = one(*split[0])
    for cut in split[1:]:
        factor_of = factor_of * one(*cut)
    return factor_of


def noise(own_key, extent, scale, bound, split=(), held_as=jnp.bfloat16):
    loudness = shard_levels(own_key, extent, split, -0.22, 0.18) if split else 1.0
    values = jax.random.normal(own_key, extent, jnp.float32) * scale * loudness
    return jnp.minimum(jnp.maximum(values, -bound), bound).astype(held_as)


def setup_inputs(seed: int = 0) -> dict:
    splits = jax.random.split(jax.random.key(seed), 19)
    return {
        "tokens": noise(splits[0], (TOKENS, D), 1.0, 6.0, ((0, 8),)),
        "cotangent": noise(splits[1], (TOKENS, D), 1.0, 6.0, ((0, 8),)),
        "counts": draw_counts(jax.random.fold_in(splits[18], 71), 0),
        "sides": draw_sides(jax.random.fold_in(splits[18], 71), 0),
        "segments": draw_segments(jax.random.fold_in(splits[18], 71), 0),
        "norm1_gain": jnp.clip(jax.random.uniform(splits[5], (D,), jnp.float32, 0.5, 1.5), 0.5, 1.5),
        "norm1_shift": noise(splits[6], (D,), 0.5, 3.0, (), jnp.float32),
        "w_qkv": noise(splits[7], (D, 3, D), D ** -0.5, 0.21875, ((2, 4),)),
        "b_qkv": noise(splits[8], (3, D), 0.5, 3.0, ((1, 4),), jnp.float32),
        "freqs": noise(splits[9], (H, 2, HD // 2), 0.5, 2.0, ((0, 4),), jnp.float32),
        "w_out": noise(splits[10], (D, D), (HD // 4) ** -0.5, 1.5, ((0, 4),)),
        "b_out": noise(splits[11], (D,), 0.5, 3.0, (), jnp.float32),
        "norm2_gain": jnp.clip(jax.random.uniform(splits[12], (D,), jnp.float32, 0.5, 1.5), 0.5, 1.5),
        "norm2_shift": noise(splits[13], (D,), 0.5, 3.0, (), jnp.float32),
        "w_fc1": noise(splits[14], (D, FF), D ** -0.5, 0.21875, ((1, 4),)),
        "b_fc1": noise(splits[15], (FF,), 0.5, 3.0, ((0, 4),), jnp.float32),
        "w_fc2": noise(splits[16], (FF, D), FF ** -0.5, 0.109375, ((0, 4),)),
        "b_fc2": noise(splits[17], (D,), 0.5, 3.0, (), jnp.float32),
    }


@jax.custom_vjp
def low(v):
    return lax.optimization_barrier(v.astype(jnp.bfloat16)).astype(jnp.float32)

@jax.custom_vjp
def low_back(v):
    return v

def low_keep(v):
    return (low(v), None)

def low_pass(kept, grad):
    return (grad,)

def back_keep(v):
    return (v, None)

def back_low(kept, grad):
    return (low(grad),)
low.defvjp(low_keep, low_pass)
low_back.defvjp(back_keep, back_low)
highest = lax.Precision.HIGHEST

def layer_norm(values_in, norm_gain, norm_shift):
    center = values_in - lax.optimization_barrier(jnp.mean(values_in, axis=-1, keepdims=True))
    spread = lax.optimization_barrier(jnp.mean(center * center, axis=-1, keepdims=True))
    return center * lax.rsqrt(spread + 1e-06) * norm_gain + norm_shift

def positions(segment_ids, image_counts, image_sides):
    slot_count = image_counts.shape[0]
    starts = jnp.cumsum(image_counts, dtype=jnp.int32) - image_counts
    matched = segment_ids[:, None] == jnp.arange(slot_count, dtype=jnp.int32)[None, :]
    start_tok = lax.optimization_barrier(jnp.sum(jnp.where(matched, starts[None, :], 0), axis=1)).astype(jnp.int32)
    side_tok = lax.optimization_barrier(jnp.sum(jnp.where(matched, image_sides[None, :], 0), axis=1)).astype(jnp.int32)
    live_slot = segment_ids < slot_count
    slot_index = jnp.arange(segment_ids.shape[0], dtype=jnp.int32)
    patch_index = jnp.where(live_slot, slot_index - start_tok, 0).astype(jnp.int32)
    side_tok = jnp.where(live_slot, side_tok, 1).astype(jnp.int32)
    row_index = patch_index // side_tok
    col_index = patch_index - row_index * side_tok
    return (col_index.astype(jnp.float32), row_index.astype(jnp.float32))

def rotate_pairs(rotate_in, freq_table, col_pos, row_pos):
    half_size = rotate_in.shape[-1] // 2
    angles = col_pos[:, None, None] * freq_table[None, :, 0, :] + row_pos[:, None, None] * freq_table[None, :, 1, :]
    cosine = jnp.cos(angles)[:, None]
    sine_part = jnp.sin(angles)[:, None]
    first_half = rotate_in[..., :half_size]
    second_half = rotate_in[..., half_size:]
    return jnp.concatenate([first_half * cosine - second_half * sine_part, first_half * sine_part + second_half * cosine], axis=-1)

def attend_forward(queries, keys, values_v, segment_ids, block_rows):
    row_total, head_count, head_size = queries.shape
    score_scale = head_size ** (-0.5)

    def one_block(pieces):
        query_blk, segment_blk = pieces
        scores = low_back(score_scale * jnp.einsum('qhd,khd->hqk', query_blk, keys, precision=highest))
        allowed = segment_blk[:, None] == segment_ids[None, :]
        scores = jnp.where(allowed[None], scores, -1e+30)
        row_top = lax.optimization_barrier(jnp.max(scores, axis=-1, keepdims=True))
        exponent = jnp.exp(scores - row_top)
        soft_weights = exponent / lax.optimization_barrier(jnp.sum(exponent, axis=-1, keepdims=True))
        return jnp.einsum('hqk,khd->qhd', low(soft_weights), values_v, precision=highest)
    blocks = (queries.reshape(row_total // block_rows, block_rows, head_count, head_size), segment_ids.reshape(row_total // block_rows, block_rows))
    mixed_heads = lax.map(jax.checkpoint(one_block), blocks)
    return mixed_heads.reshape(row_total, head_count * head_size)

def block_forward(param_set, residual, col_pos, row_pos, segment_ids):
    gain_one, shift_one, weight_qkv, bias_qkv, freq_table, weight_out, bias_out, gain_two, shift_two, weight_fc1, bias_fc1, weight_fc2, bias_fc2 = param_set
    row_total = residual.shape[0]
    head_count = freq_table.shape[0]
    head_size = residual.shape[1] // head_count
    normed_one = low(layer_norm(residual, gain_one, shift_one))
    projected = low_back(jnp.einsum('td,dcj->tcj', normed_one, weight_qkv, precision=highest) + bias_qkv[None])
    turned = rotate_pairs(projected[:, :2].reshape(row_total, 2, head_count, head_size), freq_table, col_pos, row_pos)
    queries = low(turned[:, 0])
    keys = low(turned[:, 1])
    values_v = low(projected[:, 2].reshape(row_total, head_count, head_size))
    block_rows = min(512, row_total)
    mixed_heads = low(low_back(attend_forward(queries, keys, values_v, segment_ids, block_rows)))
    branch = low_back(jnp.dot(mixed_heads, weight_out, precision=highest) + bias_out)
    middle = residual + branch
    normed_two = low(layer_norm(middle, gain_two, shift_two))
    hidden_pre = low_back(jnp.dot(normed_two, weight_fc1, precision=highest) + bias_fc1)
    hidden = low(jax.nn.gelu(hidden_pre, approximate=False))
    return middle + low_back(jnp.dot(hidden, weight_fc2, precision=highest) + bias_fc2)

def reference(tokens, cotangent, counts, sides, segments, norm1_gain, norm1_shift, w_qkv, b_qkv, freqs, w_out, b_out, norm2_gain, norm2_shift, w_fc1, b_fc1, w_fc2, b_fc2):
    residual_all = tokens.astype(jnp.float32).reshape(PACKS, PACK, D)
    segment_all = segments.reshape(PACKS, PACK)
    col_all, row_all = jax.vmap(positions)(segment_all, counts, sides)
    param_set = (norm1_gain.astype(jnp.float32), norm1_shift.astype(jnp.float32), w_qkv.astype(jnp.float32), b_qkv.astype(jnp.float32), freqs.astype(jnp.float32), w_out.astype(jnp.float32), b_out.astype(jnp.float32), norm2_gain.astype(jnp.float32), norm2_shift.astype(jnp.float32), w_fc1.astype(jnp.float32), b_fc1.astype(jnp.float32), w_fc2.astype(jnp.float32), b_fc2.astype(jnp.float32))

    def forward(params_in, residual_in):

        def apply_pack(pieces):
            return block_forward(params_in, pieces[0], pieces[1], pieces[2], pieces[3])
        return lax.map(apply_pack, (residual_in, col_all, row_all, segment_all))
    outputs, pullback = jax.vjp(forward, param_set, residual_all)
    param_grads, residual_grad = pullback(cotangent.astype(jnp.float32).reshape(PACKS, PACK, D))
    return (outputs.reshape(TOKENS, D).astype(jnp.bfloat16), residual_grad.reshape(TOKENS, D), param_grads[0], param_grads[1], param_grads[2], param_grads[3], param_grads[4], param_grads[5], param_grads[6], param_grads[7], param_grads[8], param_grads[9], param_grads[10], param_grads[11], param_grads[12])
```

```python
import jax
import jax.numpy as jnp
from jax import lax
from jax.experimental import pallas as pl
from jax.experimental.pallas import tpu as pltpu
from jax.sharding import PartitionSpec as P

BLK = 256
F32 = jnp.float32
BF16 = jnp.bfloat16
NN = (((1,), (0,)), ((), ()))
NT = (((1,), (1,)), ((), ()))
TN = (((0,), (0,)), ((), ()))

CORE, XBIT = 1, 2
ACT, WGT = CORE, XBIT


def dot(a, b, dims=NN):
    return lax.dot_general(a, b, dims, preferred_element_type=F32)


def stats(v):
    center = v - jnp.mean(v, axis=-1, keepdims=True)
    inverse = lax.rsqrt(jnp.mean(center * center, axis=-1, keepdims=True) + 1e-06)
    return center * inverse, inverse


def norm_back(grad, z, inverse, gain):
    e = grad * gain
    return inverse * (
        e - jnp.mean(e, axis=-1, keepdims=True) - z * jnp.mean(e * z, axis=-1, keepdims=True)
    )


def locate(slot, pack, cnt_ref, side_ref):
    seg = jnp.zeros_like(slot)
    start = jnp.zeros_like(slot)
    side = jnp.ones_like(slot)
    end = jnp.int32(0)
    for j in range(cnt_ref.shape[1]):
        begin, end = end, end + cnt_ref[pack, j]
        inside = (slot >= begin) & (slot < end)
        start = jnp.where(inside, begin, start)
        side = jnp.where(inside, side_ref[pack, j], side)
        seg = seg + jnp.where(slot >= end, 1, 0)
    live = seg < cnt_ref.shape[1]
    patch = jnp.where(live, slot - start, 0).astype(F32)
    side = side.astype(F32)
    row = jnp.floor((patch + 0.5) / side)
    return seg, patch - row * side, row


def angle_table(freq, lane):
    angle = freq * (lane & 31).astype(F32)
    both = jnp.concatenate([jnp.cos(angle), jnp.sin(angle)], axis=0)
    lanes = jnp.concatenate([lane, lane], axis=0)
    high = both.astype(BF16).astype(F32)
    rest = both - high
    mid = rest.astype(BF16).astype(F32)
    low = rest - mid
    picked = jnp.where(
        lanes < 32, high, jnp.where(lanes < 64, mid, jnp.where(lanes < 96, low, 0.0))
    )
    return picked.astype(BF16)


def params(name, steps=1, vmem=None):
    return pltpu.CompilerParams(dimension_semantics=("arbitrary",), vmem_limit_bytes=vmem)


def cost(flops, nbytes, trans=0):
    return pl.CostEstimate(flops=int(flops), bytes_accessed=int(nbytes), transcendentals=int(trans))


def shape(s, d):
    return jax.ShapeDtypeStruct(s, d)


def full(arr_shape):
    return pl.BlockSpec(arr_shape, lambda i, *_: (0,) * len(arr_shape))


def attend_forward(meta, counts, sides, tokens, gain, shift, w_t, small, w_out, prev):
    rows = tokens.shape[0] // counts.shape[0]
    width = tokens.shape[1]
    wide, local = w_t.shape[0], w_out.shape[0]
    heads = local // 64
    half_rows = heads * 32
    nb = rows // BLK
    hb = nb // 2
    first = prev is None

    def q_block(j, meta):
        return jnp.where(j < hb, (1 - meta[1]) * hb + j, meta[1] * hb + j - hb)

    def kernel(meta_ref, cnt_ref, sd_ref, tok_ref, gain_ref, shift_ref, w_ref, small_ref, wout_ref, *rest):
        if first:
            n1_ref, qkv_ref, lse_ref, ho_ref, cs_ref, part_ref, k3, segk, bias, tabs = rest
        else:
            prev_ref, qkv_ref, lse_ref, ho_ref, cs_ref, send_ref, keep_ref, k3, segk, bias, tabs = rest
        i = pl.program_id(0)
        pack = meta_ref[0]

        @pl.when(i == 0)
        def _():
            seg = locate(
                lax.broadcasted_iota(jnp.int32, (rows, 128), 0), pack, cnt_ref, sd_ref
            )[0]
            segk[...] = seg
            cols = jnp.transpose(small_ref[...])
            bias[...] = cols
            lane = lax.broadcasted_iota(jnp.int32, (half_rows, 128), 1)
            tabs[0] = angle_table(cols[:half_rows, 3:4], lane)
            tabs[1] = angle_table(cols[:half_rows, 4:5], lane)

        @pl.when(i < nb)
        def _():
            at = pl.ds(pl.multiple_of(i * BLK, BLK), BLK)
            slot = lax.broadcasted_iota(jnp.int32, (1, BLK), 1) + i * BLK
            _, col, row = locate(slot, pack, cnt_ref, sd_ref)
            z, _ = stats(tok_ref[...].astype(F32))
            n1 = (z * gain_ref[...] + shift_ref[...]).astype(BF16)
            if first:
                n1_ref[...] = n1
            place = (lax.broadcasted_iota(jnp.int32, (128, BLK), 0) & 31).astype(F32)
            hot_c = jnp.where(place == col, 1.0, 0.0).astype(BF16)
            hot_r = jnp.where(place == row, 1.0, 0.0).astype(BF16)
            by_col = dot(tabs[0], hot_c)
            by_row = dot(tabs[1], hot_r)
            cc, sc = by_col[:half_rows], by_col[half_rows:]
            cr, sr = by_row[:half_rows], by_row[half_rows:]
            cosine = cc * cr - sc * sr
            sine = sc * cr + cc * sr
            cs_ref[:half_rows, at] = cosine
            cs_ref[half_rows:, at] = sine
            proj = dot(w_ref[...], n1, NT)
            for c in range(3):
                for h in range(heads):
                    r = c * local + h * 64
                    u = proj[r : r + 32] + bias[h * 64 : h * 64 + 32, c : c + 1]
                    w = proj[r + 32 : r + 64] + bias[h * 64 + 32 : h * 64 + 64, c : c + 1]
                    if c < 2:
                        cs = cosine[h * 32 : h * 32 + 32]
                        sn = sine[h * 32 : h * 32 + 32]
                        u, w = u * cs - w * sn, u * sn + w * cs
                    both = jnp.concatenate([u, w], axis=0)
                    if c == 0:
                        both = both * 0.125
                    qkv_ref[r : r + 64, at] = both.astype(BF16)
                    if c == 1:
                        k3[h, at, :] = jnp.transpose(both).astype(BF16)

        @pl.when(i >= nb)
        def _():
            j = i - nb
            qb = q_block(j, meta_ref)
            at = pl.ds(pl.multiple_of(qb * BLK, BLK), BLK)
            slot = lax.broadcasted_iota(jnp.int32, (1, BLK), 1) + qb * BLK
            segq = locate(slot, pack, cnt_ref, sd_ref)[0]
            sk = jnp.concatenate([segk[...]] * (BLK // 128), axis=1)
            outs = []
            for h in range(heads):
                s = dot(k3[h], qkv_ref[h * 64 : h * 64 + 64, at])
                s = jnp.where(sk == segq, s, -1e30)
                top = jnp.max(s, axis=0, keepdims=True)
                p = jnp.exp(s - top)
                total = jnp.sum(p, axis=0, keepdims=True)
                r = 2 * local + h * 64
                o = dot(qkv_ref[r : r + 64, :], p.astype(BF16)) / total
                outs.append(o)
                lse_ref[h : h + 1, at] = top + jnp.log(total)
            o = jnp.concatenate(outs, axis=0)
            ho_ref[:, at] = o.astype(BF16)
            part = dot(jnp.transpose(o).astype(BF16), wout_ref[...])
            if first:
                part_ref[...] = part
            else:
                part = part + prev_ref[...]

                @pl.when(j < hb)
                def _():
                    send_ref[...] = part.astype(BF16)

                @pl.when(j >= hb)
                def _():
                    keep_ref[...] = part

    def tok_map(i, meta, *_):
        return (meta[0] * nb + jnp.minimum(i, nb - 1), 0)

    def q_map(i, meta, *_):
        return (q_block(jnp.maximum(i - nb, 0), meta), 0)

    in_specs = [
        pl.BlockSpec((BLK, width), tok_map),
        full((1, width)),
        full((1, width)),
        full(w_t.shape),
        full(small.shape),
        full(w_out.shape),
    ]
    operands = [tokens, gain, shift, w_t, small, w_out]
    common_out = [
        (shape((wide, rows), BF16), full((wide, rows))),
        (shape((8, rows), F32), full((8, rows))),
        (shape((local, rows), BF16), full((local, rows))),
        (shape((2 * half_rows, rows), F32), full((2 * half_rows, rows))),
    ]
    if first:
        outs = (
            [(shape((rows, width), BF16), pl.BlockSpec((BLK, width), lambda i, *_: (jnp.minimum(i, nb - 1), 0)))]
            + common_out
            + [(shape((rows, width), F32), pl.BlockSpec((BLK, width), q_map))]
        )
    else:
        in_specs.append(pl.BlockSpec((BLK, width), q_map))
        operands.append(prev)
        outs = common_out + [
            (shape((rows // 2, width), BF16), pl.BlockSpec((BLK, width), lambda i, *_: (jnp.clip(i - nb, 0, hb - 1), 0))),
            (shape((rows // 2, width), F32), pl.BlockSpec((BLK, width), lambda i, *_: (jnp.clip(i - nb - hb, 0, hb - 1), 0))),
        ]
    return pl.pallas_call(
        kernel,
        name="attn_fwd",
        out_shape=[o[0] for o in outs],
        grid_spec=pltpu.PrefetchScalarGridSpec(
            num_scalar_prefetch=3,
            grid=(2 * nb,),
            in_specs=in_specs,
            out_specs=[o[1] for o in outs],
            scratch_shapes=[
                pltpu.VMEM((heads, rows, 64), BF16),
                pltpu.VMEM((rows, 128), jnp.int32),
                pltpu.VMEM((256, 8), F32),
                pltpu.VMEM((2, 2 * half_rows, 128), BF16),
            ],
        ),
        compiler_params=params("attn_fwd"),
        cost_estimate=cost(
            2 * rows * width * (wide + local) + 16 * rows * rows * 64 * heads,
            6 * rows * width + 2 * wide * (rows + width),
            rows * rows * heads,
        ),
    )(meta, counts, sides, *operands)


def middle_norm(meta, tokens, keep, recv, b_out, gain, shift):
    rows, width = keep.shape

    def kernel(meta_ref, tok_ref, keep_ref, recv_ref, b_ref, gain_ref, shift_ref, mid_ref, n2_ref):
        mid = tok_ref[...].astype(F32) + (keep_ref[...] + recv_ref[...].astype(F32)) + b_ref[...]
        z, _ = stats(mid)
        mid_ref[...] = mid
        n2_ref[...] = (z * gain_ref[...] + shift_ref[...]).astype(BF16)

    blk = pl.BlockSpec((BLK, width), lambda i, *_: (i, 0))
    return pl.pallas_call(
        kernel,
        name="middle_norm",
        out_shape=[shape((rows, width), F32), shape((rows, width), BF16)],
        grid_spec=pltpu.PrefetchScalarGridSpec(
            num_scalar_prefetch=1,
            grid=(rows // BLK,),
            in_specs=[
                pl.BlockSpec((BLK, width), lambda i, meta: (meta[2] + i, 0)),
                blk,
                blk,
                full((1, width)),
                full((1, width)),
                full((1, width)),
            ],
            out_specs=[blk, blk],
        ),
        compiler_params=params("middle_norm"),
        cost_estimate=cost(20 * rows * width, 14 * rows * width),
    )(meta, tokens, keep, recv, b_out, gain, shift)


def gelu_parts(x):
    a = jnp.abs(x)
    t = 1.0 / (1.0 + (0.3275911 * 0.7071067811865476) * a)
    e = jnp.exp(-0.5 * (x * x))
    poly = ((((1.061405429 * t - 1.453152027) * t + 1.421413741) * t - 0.284496736) * t + 0.254829592) * t
    half = 0.5 * (poly * e)
    up = x >= 0
    gelu = jnp.maximum(x, 0.0) - a * half
    slope = jnp.where(up, 1.0 - half, half) + x * (0.3989422804014327 * e)
    return gelu, slope


def mlp_rows(meta, where, n2, cot, w1s, b1s, w2s, out_type):
    rows, width = n2.shape
    ff = w1s[0].shape[1]

    def kernel(meta_ref, n2_ref, cot_ref, w1a, w1b, b1a, b1b, w2a, w2b, ha, hb, da, db, dn_ref):
        n2v = n2_ref[...]
        cv = cot_ref[...]
        total = None
        for w1, b1, w2, h_ref, d_ref in ((w1a, b1a, w2a, ha, da), (w1b, b1b, w2b, hb, db)):
            pre = dot(n2v, w1[...]) + b1[...]
            grad = dot(cv, w2[...], NT)
            gelu, slope = gelu_parts(pre)
            h_ref[...] = gelu.astype(BF16)
            d = (grad * slope).astype(BF16)
            d_ref[...] = d
            part = dot(d, w1[...], NT)
            total = part if total is None else total + part
        dn_ref[...] = total.astype(out_type)

    blk = pl.BlockSpec((BLK, width), lambda i, *_: (i, 0))
    fblk = pl.BlockSpec((BLK, ff), lambda i, *_: (i, 0))
    return pl.pallas_call(
        kernel,
        name="mlp_rows",
        out_shape=[shape((rows, ff), BF16)] * 4 + [shape((rows, width), out_type)],
        grid_spec=pltpu.PrefetchScalarGridSpec(
            num_scalar_prefetch=1,
            grid=(rows // BLK,),
            in_specs=[
                blk,
                pl.BlockSpec((BLK, width), lambda i, meta: (meta[where] + i, 0)),
                full((width, ff)),
                full((width, ff)),
                full((1, ff)),
                full((1, ff)),
                full((ff, width)),
                full((ff, width)),
            ],
            out_specs=[fblk] * 4 + [blk],
        ),
        compiler_params=params("mlp_rows"),
        cost_estimate=cost(12 * rows * width * ff, 8 * width * ff + 14 * rows * width, 4 * rows * ff),
    )(meta, n2, cot, w1s[0], w1s[1], b1s[0], b1s[1], w2s[0], w2s[1])


def mlp_out(hidden_own, hidden_peer, w2s):
    rows, ff = hidden_own[0].shape
    width = w2s[0].shape[1]

    def kernel(oa, ob, pa, pb, w2a, w2b, keep_ref, send_ref):
        send_ref[...] = (dot(pa[...], w2a[...]) + dot(pb[...], w2b[...])).astype(BF16)
        keep_ref[...] = dot(oa[...], w2a[...]) + dot(ob[...], w2b[...])

    fblk = pl.BlockSpec((BLK, ff), lambda i: (i, 0))
    blk = pl.BlockSpec((BLK, width), lambda i: (i, 0))
    return pl.pallas_call(
        kernel,
        name="mlp_out",
        grid=(rows // BLK,),
        out_shape=[shape((rows, width), F32), shape((rows, width), BF16)],
        in_specs=[fblk] * 4 + [full((ff, width))] * 2,
        out_specs=[blk, blk],
        compiler_params=params("mlp_out"),
        cost_estimate=cost(8 * rows * width * ff, 4 * width * ff + 14 * rows * width),
    )(*hidden_own, *hidden_peer, *w2s)


def mlp_weights(meta, n2s, cot, hidden_own, hidden_peer, pre_own, pre_peer):
    rows, width = n2s[0].shape
    ff = hidden_own[0].shape[1]
    steps = width // BLK

    def kernel(meta_ref, n2o, n2p, co, cp, hoa, hob, hpa, hpb, doa, dob, dpa, dpb, k1, k2, s1, s2, bias):
        i = pl.program_id(0)
        k1[...] = dot(n2o[...], doa[...], TN) + dot(n2p[...], dpa[...], TN)
        s1[...] = (dot(n2o[...], dob[...], TN) + dot(n2p[...], dpb[...], TN)).astype(BF16)
        k2[...] = dot(hoa[...], co[...], TN) + dot(hpa[...], cp[...], TN)
        s2[...] = (dot(hob[...], co[...], TN) + dot(hpb[...], cp[...], TN)).astype(BF16)

        @pl.when(i == 0)
        def _():
            own = jnp.sum(doa[...].astype(F32), axis=0, keepdims=True) + jnp.sum(
                dpa[...].astype(F32), axis=0, keepdims=True
            )
            peer = jnp.sum(dob[...].astype(F32), axis=0, keepdims=True) + jnp.sum(
                dpb[...].astype(F32), axis=0, keepdims=True
            )
            bias[...] = jnp.concatenate([own, peer, jnp.zeros((6, ff), F32)], axis=0)

    nblk = pl.BlockSpec((rows, BLK), lambda i, *_: (0, i))
    out = pl.BlockSpec((BLK, ff), lambda i, *_: (i, 0))
    per = rows // BLK
    return pl.pallas_call(
        kernel,
        name="mlp_weights",
        out_shape=[shape((width, ff), F32), shape((ff, width), F32), shape((width, ff), BF16), shape((ff, width), BF16), shape((8, ff), F32)],
        grid_spec=pltpu.PrefetchScalarGridSpec(
            num_scalar_prefetch=1,
            grid=(steps,),
            in_specs=[
                nblk,
                nblk,
                pl.BlockSpec((rows, width), lambda i, meta: (meta[2] // per, 0)),
                pl.BlockSpec((rows, width), lambda i, meta: (meta[3] // per, 0)),
                nblk,
                nblk,
                nblk,
                nblk,
                full((rows, ff)),
                full((rows, ff)),
                full((rows, ff)),
                full((rows, ff)),
            ],
            out_specs=[out, out, out, out, full((8, ff))],
        ),
        compiler_params=params("mlp_weights"),
        cost_estimate=cost(16 * rows * width * ff, 12 * width * ff + 24 * rows * width),
    )(meta, n2s[0], n2s[1], cot, cot, *hidden_own, *hidden_peer, *pre_own, *pre_peer)


def norm_two_back(meta, middle, keep, recv, cot, gain):
    rows, width = middle.shape

    def kernel(meta_ref, mid_ref, keep_ref, recv_ref, cot_ref, gain_ref, dm_ref, db_ref, sums):
        @pl.when(pl.program_id(0) == 0)
        def _():
            sums[...] = jnp.zeros_like(sums)

        z, inverse = stats(mid_ref[...])
        dn = keep_ref[...] + recv_ref[...].astype(F32)
        dy = cot_ref[...].astype(F32)
        dm = dy + norm_back(dn, z, inverse, gain_ref[...])
        low = dm.astype(BF16)
        dm_ref[...] = dm
        db_ref[...] = low
        for n, v in enumerate((dn * z, dn, low.astype(F32), dy)):
            sums[n : n + 1, :] += jnp.sum(v, axis=0, keepdims=True)

    blk = pl.BlockSpec((BLK, width), lambda i, *_: (i, 0))
    return pl.pallas_call(
        kernel,
        name="norm_two_back",
        out_shape=[shape((rows, width), F32), shape((rows, width), BF16), shape((8, width), F32)],
        grid_spec=pltpu.PrefetchScalarGridSpec(
            num_scalar_prefetch=1,
            grid=(rows // BLK,),
            in_specs=[blk, blk, blk, pl.BlockSpec((BLK, width), lambda i, meta: (meta[2] + i, 0)), full((1, width))],
            out_specs=[blk, blk, full((8, width))],
        ),
        compiler_params=params("norm_two_back"),
        cost_estimate=cost(30 * rows * width, 18 * rows * width),
    )(meta, middle, keep, recv, cot, gain)


def attend_backward(meta, counts, sides, d_own, d_peer, qkv, lse, ho, cs, w_out, out_type):
    rows = qkv.shape[1]
    wide, local = qkv.shape[0], w_out.shape[0]
    width = w_out.shape[1]
    heads = local // 64
    half_rows = heads * 32
    nb = rows // BLK
    hb = nb // 2

    def kernel(
        meta_ref, cnt_ref, sd_ref, down_ref, dpeer_ref, qkv_ref, lse_ref, ho_ref, cs_ref, wout_ref,
        dp_ref, dwo_ref, small_ref, k3, v3, segk, dk, dv, dwo, fc, fr, cols,
    ):
        i = pl.program_id(0)
        pack = meta_ref[0]

        @pl.when(i == 0)
        def _():
            segk[...] = locate(
                lax.broadcasted_iota(jnp.int32, (rows, 128), 0), pack, cnt_ref, sd_ref
            )[0]
            for h in range(heads):
                r = local + h * 64
                k3[h] = jnp.transpose(qkv_ref[r : r + 64, :].astype(F32)).astype(BF16)
                r = 2 * local + h * 64
                v3[h] = jnp.transpose(qkv_ref[r : r + 64, :].astype(F32)).astype(BF16)
            dk[...] = jnp.zeros_like(dk)
            dv[...] = jnp.zeros_like(dv)
            dwo[...] = jnp.zeros_like(dwo)
            fc[...] = jnp.zeros_like(fc)
            fr[...] = jnp.zeros_like(fr)

        @pl.when(i < nb)
        def _():
            qb = jnp.where(i < hb, meta_ref[1] * hb + i, (1 - meta_ref[1]) * hb + i - hb)
            at = pl.ds(pl.multiple_of(qb * BLK, BLK), BLK)
            slot = lax.broadcasted_iota(jnp.int32, (1, BLK), 1) + qb * BLK
            segq, col, row = locate(slot, pack, cnt_ref, sd_ref)
            sk = jnp.concatenate([segk[...]] * (BLK // 128), axis=1)
            db = jnp.where(i < hb, down_ref[...], dpeer_ref[...])
            do = dot(wout_ref[...], db, NT)
            do_low = do.astype(BF16)
            hov = ho_ref[:, at]
            dwo[...] += dot(hov, db)
            prod = do_low.astype(F32) * hov.astype(F32)
            for h in range(heads):
                hs = slice(h * 64, h * 64 + 64)
                q = qkv_ref[hs, at]
                s = dot(k3[h], q)
                p = jnp.where(sk == segq, jnp.exp(s - lse_ref[h : h + 1, at]), 0.0)
                grad = dot(v3[h], do_low[hs])
                delta = jnp.sum(prod[hs], axis=0, keepdims=True)
                ds = (p * (grad - delta)).astype(BF16)
                low = p.astype(BF16)
                dv[hs, :] += dot(do_low[hs], low, NT)
                dk[hs, :] += dot(q, ds, NT)
                dq = dot(qkv_ref[local + h * 64 : local + h * 64 + 64, :], ds)
                cosine = cs_ref[h * 32 : h * 32 + 32, at]
                sine = cs_ref[half_rows + h * 32 : half_rows + h * 32 + 32, at]
                du, dw = dq[:32], dq[32:]
                q32 = q.astype(F32)
                cross = q32[:32] * dw - q32[32:] * du
                fc[h * 32 : h * 32 + 32, :] += cross * col
                fr[h * 32 : h * 32 + 32, :] += cross * row
                back = jnp.concatenate([du * cosine + dw * sine, dw * cosine - du * sine], axis=0)
                dp_ref[hs, at] = (back * 0.125).astype(BF16)

        @pl.when(i == nb)
        def _():
            slot = lax.broadcasted_iota(jnp.int32, (1, rows), 1)
            _, col, row = locate(slot, pack, cnt_ref, sd_ref)
            for h in range(heads):
                hs = slice(local + h * 64, local + h * 64 + 64)
                du, dw = dk[h * 64 : h * 64 + 32, :], dk[h * 64 + 32 : h * 64 + 64, :]
                cosine = cs_ref[h * 32 : h * 32 + 32, :]
                sine = cs_ref[half_rows + h * 32 : half_rows + h * 32 + 32, :]
                k32 = qkv_ref[hs, :].astype(F32)
                cross = k32[:32] * dw - k32[32:] * du
                fs = slice(h * 32, h * 32 + 32)
                cols[fs, 3:4] = jnp.sum(cross * col, axis=1, keepdims=True) + jnp.sum(fc[fs, :], axis=1, keepdims=True)
                cols[fs, 4:5] = jnp.sum(cross * row, axis=1, keepdims=True) + jnp.sum(fr[fs, :], axis=1, keepdims=True)
                back = jnp.concatenate([du * cosine + dw * sine, dw * cosine - du * sine], axis=0)
                dp_ref[hs, :] = back.astype(BF16)
            dp_ref[2 * local :, :] = dv[...].astype(BF16)
            for c in range(3):
                cols[0:local, c : c + 1] = jnp.sum(
                    dp_ref[c * local : (c + 1) * local, :].astype(F32), axis=1, keepdims=True
                )
            small_ref[...] = jnp.transpose(cols[...])[:8]
            dwo_ref[...] = dwo[...].astype(out_type)

    clip = lambda v: jnp.clip(v, 0, hb - 1)
    return pl.pallas_call(
        kernel,
        name="attn_bwd",
        out_shape=[shape((wide, rows), BF16), shape((local, width), out_type), shape((8, 256), F32)],
        grid_spec=pltpu.PrefetchScalarGridSpec(
            num_scalar_prefetch=3,
            grid=(nb + 1,),
            in_specs=[
                pl.BlockSpec((BLK, width), lambda i, *_: (clip(i), 0)),
                pl.BlockSpec((BLK, width), lambda i, *_: (clip(i - hb), 0)),
                full((wide, rows)),
                full((8, rows)),
                full((local, rows)),
                full((2 * half_rows, rows)),
                full((local, width)),
            ],
            out_specs=[full((wide, rows)), full((local, width)), full((8, 256))],
            scratch_shapes=[
                pltpu.VMEM((heads, rows, 64), BF16),
                pltpu.VMEM((heads, rows, 64), BF16),
                pltpu.VMEM((rows, 128), jnp.int32),
                pltpu.VMEM((local, rows), F32),
                pltpu.VMEM((local, rows), F32),
                pltpu.VMEM((local, width), F32),
                pltpu.VMEM((half_rows, BLK), F32),
                pltpu.VMEM((half_rows, BLK), F32),
                pltpu.VMEM((256, 128), F32),
            ],
        ),
        compiler_params=params("attn_bwd"),
        cost_estimate=cost(
            40 * rows * rows * 64 * heads + 4 * rows * width * local,
            4 * wide * rows + 2 * rows * width + 6 * local * width,
            rows * rows * heads,
        ),
    )(meta, counts, sides, d_own, d_peer, qkv, lse, ho, cs, w_out)


def input_grads(meta, d_own, d_peer, w_own, w_peer):
    wide, rows = d_own.shape
    width = w_own.shape[1]
    nb = rows // BLK
    hb = nb // 2

    def kernel(meta_ref, da, db, wa, wb, send_ref, keep_ref):
        i = pl.program_id(0)
        v = dot(da[...], wa[...], TN) + dot(db[...], wb[...], TN)

        @pl.when(i < hb)
        def _():
            send_ref[...] = v.astype(BF16)

        @pl.when(i >= hb)
        def _():
            keep_ref[...] = v

    def blk_map(i, meta):
        return (0, jnp.where(i < hb, (1 - meta[1]) * hb + i, meta[1] * hb + i - hb))

    return pl.pallas_call(
        kernel,
        name="input_grads",
        out_shape=[shape((rows // 2, width), BF16), shape((rows // 2, width), F32)],
        grid_spec=pltpu.PrefetchScalarGridSpec(
            num_scalar_prefetch=1,
            grid=(nb,),
            in_specs=[
                pl.BlockSpec((wide, BLK), blk_map),
                pl.BlockSpec((wide, BLK), blk_map),
                full((wide, width)),
                full((wide, width)),
            ],
            out_specs=[
                pl.BlockSpec((BLK, width), lambda i, *_: (jnp.clip(i, 0, hb - 1), 0)),
                pl.BlockSpec((BLK, width), lambda i, *_: (jnp.clip(i - hb, 0, hb - 1), 0)),
            ],
        ),
        compiler_params=params("input_grads"),
        cost_estimate=cost(4 * rows * width * wide, 4 * wide * (rows + width) + 3 * rows * width),
    )(meta, d_own, d_peer, w_own, w_peer)


def attn_weights(d_own, d_peer, n1, dwo_own, dwo_peer):
    wide, rows = d_own.shape
    width = n1.shape[1]
    local = dwo_own.shape[0]

    def kernel(da, db, n1_ref, oa, ob, keep_ref, send_ref):
        send_ref[:wide] = dot(db[...], n1_ref[...]).astype(BF16)
        send_ref[wide:] = ob[...]
        keep_ref[:wide] = dot(da[...], n1_ref[...])
        keep_ref[wide:] = oa[...]

    col = lambda r: pl.BlockSpec((r, BLK), lambda i: (0, i))
    return pl.pallas_call(
        kernel,
        name="attn_weights",
        grid=(width // BLK,),
        out_shape=[shape((wide + local, width), F32), shape((wide + local, width), BF16)],
        in_specs=[full((wide, rows)), full((wide, rows)), col(rows), col(local), col(local)],
        out_specs=[col(wide + local), col(wide + local)],
        compiler_params=params("attn_weights"),
        cost_estimate=cost(4 * rows * width * wide, 4 * wide * rows + 2 * rows * width + 6 * (wide + local) * width),
    )(d_own, d_peer, n1, dwo_own, dwo_peer)


def norm_one_back(meta, tokens, keep, recv, d_middle, gain):
    rows, width = d_middle.shape

    def kernel(meta_ref, tok_ref, keep_ref, recv_ref, dm_ref, gain_ref, out_ref, sums):
        @pl.when(pl.program_id(0) == 0)
        def _():
            sums[...] = jnp.zeros_like(sums)

        z, inverse = stats(tok_ref[...].astype(F32))
        dn = keep_ref[...] + recv_ref[...].astype(F32)
        out_ref[...] = (dm_ref[...] + norm_back(dn, z, inverse, gain_ref[...])).astype(BF16)
        sums[0:1, :] += jnp.sum(dn * z, axis=0, keepdims=True)
        sums[1:2, :] += jnp.sum(dn, axis=0, keepdims=True)

    blk = pl.BlockSpec((BLK, width), lambda i, *_: (i, 0))
    return pl.pallas_call(
        kernel,
        name="norm_one_back",
        out_shape=[shape((rows, width), BF16), shape((8, width), F32)],
        grid_spec=pltpu.PrefetchScalarGridSpec(
            num_scalar_prefetch=1,
            grid=(rows // BLK,),
            in_specs=[pl.BlockSpec((BLK, width), lambda i, meta: (meta[2] + i, 0)), blk, blk, blk, full((1, width))],
            out_specs=[blk, full((8, width))],
        ),
        compiler_params=params("norm_one_back"),
        cost_estimate=cost(30 * rows * width, 14 * rows * width),
    )(meta, tokens, keep, recv, d_middle, gain)


def block_rows(middle, keep, recv, b_fc2):
    rows, width = middle.shape

    def kernel(mid_ref, keep_ref, recv_ref, b_ref, out_ref):
        out_ref[...] = (mid_ref[...] + (keep_ref[...] + recv_ref[...].astype(F32)) + b_ref[...]).astype(BF16)

    blk = pl.BlockSpec((BLK, width), lambda i: (i, 0))
    return pl.pallas_call(
        kernel,
        name="block_rows",
        grid=(rows // BLK,),
        out_shape=shape((rows, width), BF16),
        in_specs=[blk, blk, blk, full((1, width))],
        out_specs=blk,
        compiler_params=params("block_rows"),
        cost_estimate=cost(4 * rows * width, 12 * rows * width),
    )(middle, keep, recv, b_fc2)


def assemble(place, parts, out_type):
    rows, width = parts[0].shape
    count = len(parts)
    per = rows // BLK

    def kernel(place_ref, *refs):
        i = pl.program_id(0)
        for n in range(count):

            @pl.when(i // per == n)
            def _():
                refs[count][...] = refs[n][...].astype(out_type)

    def spec(n):
        return pl.BlockSpec((BLK, width), lambda i, place: (jnp.clip(i - n * per, 0, per - 1), 0))

    return pl.pallas_call(
        kernel,
        name="assemble",
        out_shape=shape((rows * count, width), out_type),
        grid_spec=pltpu.PrefetchScalarGridSpec(
            num_scalar_prefetch=1,
            grid=(per * count,),
            in_specs=[spec(n) for n in range(count)],
            out_specs=pl.BlockSpec((BLK, width), lambda i, place: (place[i // per] * per + i % per, 0)),
        ),
        compiler_params=params("assemble"),
        cost_estimate=cost(rows * width, 6 * rows * width * count),
    )(place, *parts)


def swap(v, axis, mask, count):
    return lax.ppermute(v, axis, [(i, i ^ mask) for i in range(count)])


def bits_of(count):
    masks = []
    mask = 1
    while mask < count:
        masks.append(mask)
        mask *= 2
    return masks


def reduce_over(keep, recv, index, masks, count):
    value = keep + recv.astype(F32)
    for mask in masks:
        mine = jnp.bitwise_and(index // mask, 1)
        half = value.shape[0] // 2
        send = lax.dynamic_slice_in_dim(value, (1 - mine) * half, half, 0).astype(BF16)
        stay = lax.dynamic_slice_in_dim(value, mine * half, half, 0)
        value = stay + swap(send, "dp", mask, count).astype(F32)
    value = value.astype(BF16)
    for mask in reversed(masks):
        mine = jnp.bitwise_and(index // mask, 1)
        other = swap(value, "dp", mask, count)
        value = jnp.where(
            mine == 0, jnp.concatenate([value, other], axis=0), jnp.concatenate([other, value], axis=0)
        )
    return value.astype(F32)


def solution(mesh):
    n_dp, n_tensor = mesh.shape["dp"], mesh.shape["tensor"]

    def on_device(
        tokens, cotangent, counts, sides, segments, norm1_gain, norm1_shift, w_qkv, b_qkv, freqs,
        w_out, b_out, norm2_gain, norm2_shift, w_fc1, b_fc1, w_fc2, b_fc2,
    ):
        width = tokens.shape[1]
        heads = freqs.shape[0]
        local = w_qkv.shape[2]
        ff = w_fc1.shape[1]
        per = tokens.shape[0] // 4 // BLK
        tensor = lax.axis_index("tensor")
        data = lax.axis_index("dp")
        x_bit, core_bit = tensor // 2, tensor % 2
        pack, half = (x_bit, core_bit) if ACT == CORE else (core_bit, x_bit)
        peer_pack, peer_half = (1 - x_bit, core_bit) if ACT == CORE else (core_bit, 1 - x_bit)
        meta = jnp.stack(
            [pack, half, (pack * 2 + half) * per, (peer_pack * 2 + peer_half) * per]
        ).astype(jnp.int32)
        tswap = lambda v, mask: swap(v, "tensor", mask, n_tensor)
        row = lambda v: v.reshape(1, -1)

        w_t = jnp.transpose(w_qkv, (1, 2, 0)).reshape(3 * local, width)
        small = jnp.zeros((8, 256), F32)
        small = lax.dynamic_update_slice(small, b_qkv, (0, 0))
        small = lax.dynamic_update_slice(
            small, jnp.transpose(freqs, (1, 0, 2)).reshape(2, heads * 32), (3, 0)
        )
        w_t_peer = tswap(w_t, WGT)
        small_peer = tswap(small, WGT)
        w_out_peer = tswap(w_out, WGT)
        w1s = (w_fc1, tswap(w_fc1, CORE))
        w2s = (w_fc2, tswap(w_fc2, CORE))
        b1 = row(b_fc1)
        b1s = (b1, tswap(b1, CORE))
        gain1, shift1 = row(norm1_gain), row(norm1_shift)
        gain2, shift2 = row(norm2_gain), row(norm2_shift)

        n1, qkv_a, lse_a, ho_a, cs_a, part = attend_forward(
            meta, counts, sides, tokens, gain1, shift1, w_t, small, w_out, None
        )
        qkv_b, lse_b, ho_b, cs_b, send, keep = attend_forward(
            meta, counts, sides, tokens, gain1, shift1, w_t_peer, small_peer, w_out_peer, part
        )
        recv = tswap(send, ACT)
        middle, n2 = middle_norm(meta, tokens, keep, recv, row(b_out), gain2, shift2)
        n2_peer = tswap(n2, XBIT)
        *own, dn_keep = mlp_rows(meta, 2, n2, cotangent, w1s, b1s, w2s, F32)
        *peer, dn_send = mlp_rows(meta, 3, n2_peer, cotangent, w1s, b1s, w2s, BF16)
        dn_recv = tswap(dn_send, XBIT)
        d_middle, d_own, sums2 = norm_two_back(meta, middle, dn_keep, dn_recv, cotangent, gain2)
        d_peer = tswap(d_own, ACT)

        y_keep, y_send = mlp_out(own[:2], peer[:2], w2s)
        y_recv = tswap(y_send, XBIT)
        k1, k2, s1, s2, bias1 = mlp_weights(
            meta, (n2, n2_peer), cotangent, own[:2], peer[:2], own[2:], peer[2:]
        )
        masks = bits_of(n_dp)
        g1 = reduce_over(k1, tswap(s1, CORE), data, masks, n_dp)
        g2 = reduce_over(k2, tswap(s2, CORE), data, masks[1:] + masks[:1], n_dp)
        out_own = block_rows(middle, y_keep, y_recv, row(b_fc2))

        dp_a, dwo_a, small_a = attend_backward(
            meta, counts, sides, d_own, d_peer, qkv_a, lse_a, ho_a, cs_a, w_out, F32
        )
        dp_b, dwo_b, small_b = attend_backward(
            meta, counts, sides, d_own, d_peer, qkv_b, lse_b, ho_b, cs_b, w_out_peer, BF16
        )
        d1_send, d1_keep = input_grads(meta, dp_a, dp_b, w_t, w_t_peer)
        d1_recv = tswap(d1_send, ACT)
        wk, ws = attn_weights(dp_a, dp_b, n1, dwo_a, dwo_b)
        grad_own, sums1 = norm_one_back(meta, tokens, d1_keep, d1_recv, d_middle, gain1)
        ga = reduce_over(wk, tswap(ws, WGT), data, masks, n_dp)

        spots = jnp.stack([pack * 2 + half] * 4)
        own_spot = pack * 2 + half
        x_spot = peer_pack * 2 + peer_half
        c_pack, c_half = (x_bit, 1 - core_bit) if ACT == CORE else (1 - core_bit, x_bit)
        d_pack, d_half = (1 - x_bit, 1 - core_bit) if ACT == CORE else (1 - core_bit, 1 - x_bit)
        spots = jnp.stack([own_spot, x_spot, c_pack * 2 + c_half, d_pack * 2 + d_half]).astype(jnp.int32)

        def spread(v, out_type):
            over = tswap(v, XBIT)
            return assemble(spots, [v, over, tswap(v, CORE), tswap(over, CORE)], out_type)

        block_output = spread(out_own, BF16)
        token_grad = spread(grad_own, F32)

        flat = lambda s: jnp.concatenate([s[:3, :local].reshape(-1), s[3:5, : heads * 32].reshape(-1)])
        place = lambda v, spot: jnp.where(jnp.arange(4)[:, None] == spot, v[None, :], 0.0)
        w_spot = tensor ^ WGT
        rows16 = jnp.concatenate(
            [
                sums1[:2],
                sums2[:4],
                place(bias1[0], tensor) + place(bias1[1], tensor ^ CORE),
                place(flat(small_a), tensor) + place(flat(small_b), w_spot),
                jnp.zeros((2, width), F32),
            ],
            axis=0,
        )
        for mask in bits_of(n_tensor):
            rows16 = rows16 + tswap(rows16, mask)
        for mask in masks:
            rows16 = rows16 + swap(rows16, "dp", mask, n_dp)
        fc1_bias = lax.dynamic_slice_in_dim(rows16, 6 + tensor, 1, 0)[0]
        qf = lax.dynamic_slice_in_dim(rows16, 10 + tensor, 1, 0)[0]
        qkv_bias = qf[: 3 * local].reshape(3, local)
        freqs_grad = jnp.transpose(qf[3 * local :].reshape(2, heads, 32), (1, 0, 2))
        qkv_grad = jnp.transpose(ga[: 3 * local].reshape(3, local, width), (2, 0, 1))
        return (
            block_output,
            token_grad,
            rows16[0],
            rows16[1],
            qkv_grad,
            qkv_bias,
            freqs_grad,
            ga[3 * local :],
            rows16[4],
            rows16[2],
            rows16[3],
            g1,
            fc1_bias,
            g2,
            rows16[5],
        )

    in_specs = (
        P("dp", None), P("dp", None), P("dp", None), P("dp", None), P("dp"), P(), P(),
        P(None, None, "tensor"), P(None, "tensor"), P("tensor", None, None), P("tensor", None), P(), P(), P(),
        P(None, "tensor"), P("tensor"), P("tensor", None), P(),
    )
    out_specs = (
        P("dp", None), P("dp", None), P(), P(), P(None, None, "tensor"), P(None, "tensor"), P("tensor", None, None),
        P("tensor", None), P(), P(), P(), P(None, "tensor"), P("tensor"), P("tensor", None), P(),
    )
    return jax.shard_map(on_device, mesh=mesh, in_specs=in_specs, out_specs=out_specs, check_vma=False)
```
